32 devices in a mesh: row: 4 (over y, x), col: 8 (over z, core).
Axes of the slice: x: 2, y: 2, z: 4, core: 2. Of those that a mesh axis runs over, the one named last changes fastest.
Arguments:
- patches: bfloat16 [32, 128, 768], P('row', 'col'), may hold values from -6 to 6
- w_patch: bfloat16 [768, 6144], replicated, may hold values from -0.21875 to 0.21875
- patch_bias: bfloat16 [6144], replicated, may hold values from -5 to 5
- ln_gain: bfloat16 [6144], replicated, may hold values from 0.5 to 1.5
- w_qkv: bfloat16 [6144, 3, 48, 128], P(None, None, 'col'), may hold values from -1 to 1
- qk_gain: float32 [2, 48, 128], P(None, 'col'), may hold values from 0 to 6, as said below
- w_out: bfloat16 [48, 128, 6144], P('col', None, 'row'), may hold values from -0.078125 to 0.078125
Outputs:
- attn_branch: bfloat16 [4096, 6144], P(('row', 'col'))
The draws below stay inside these ranges and needn't reach their ends.
Inputs may be any that keep to these rules, and one draw needn't show every extreme that they name: `qk_gain`: positive gains.
All inputs are finite; a program needn't handle non-finite values.
Results may differ from the reference program's by a relative error of at most 0.015.
Values may be sent and summed in bfloat16 or wider, within the bound.
A program may use at most 320 MiB of HBM per device.

```python
import math
import jax
import jax.numpy as jnp
from jax import lax

D = 6144
H = 48
HD = 128
PATCH_IN = 768
GW = 128
GH = 32
N_COL = 8


def draw_patches(key, part):
    key_one = jax.random.fold_in(key, 0)
    result = jnp.clip(jax.random.normal(key_one, (GH, GW, PATCH_IN), jnp.float32), -6.0, 6.0)
    return result.astype(jnp.bfloat16)


def draw_w_qkv(key, part):
    key_weight = jax.random.fold_in(key, 0)
    raw_draw = jnp.clip(jax.random.normal(key_weight, (D, 3, H, HD), jnp.float32), -6.0, 6.0) * D ** (-0.5)
    return raw_draw.astype(jnp.bfloat16)


def draw_qk_gain(key, part):
    key_head, key_dim = jax.random.split(key, 2)
    head_scale = jnp.exp(jax.random.uniform(key_head, (2, H, 1), jnp.float32, 0.5, 1.5))
    gains = head_scale * (1.0 + 0.1 * jnp.clip(jax.random.normal(key_dim, (2, H, HD), jnp.float32), -3.0, 3.0))
    return gains.astype(jnp.float32)


def shard_levels(key, extent, cuts, smallest, largest):
    def one(dim, shards_of):
        heights = jax.random.uniform(jax.random.fold_in(jax.random.fold_in(key, 6), dim), (shards_of,), jnp.float32, smallest / len(cuts), largest / len(cuts))
        return jnp.repeat(jnp.exp(heights), extent[dim] // shards_of).reshape((-1,) + (1,) * (len(extent) - dim - 1))

    gain = one(*cuts[0])
    for cut in cuts[1:]:
        gain = gain * one(*cut)
    return gain


def centred(stream_key, dims, spread, limit, pieces=(), held_as=jnp.bfloat16):
    entries = jax.random.normal(stream_key, dims, jnp.float32) * spread
    if len(pieces) > 0:
        entries = shard_levels(stream_key, dims, pieces, -0.22, 0.18) * entries
    return jnp.clip(entries, min=-limit, max=limit).astype(held_as)


def setup_inputs(seed: int = 0) -> dict:
    arg_keys = jax.random.split(jax.random.key(seed), 8)
    patches = draw_patches(jax.random.fold_in(arg_keys[7], 71), 0)
    w_patch = centred(arg_keys[1], (PATCH_IN, D), PATCH_IN ** -0.5, 0.21875)
    patch_bias = centred(arg_keys[2], (D,), 1.0, 5.0)
    ln_gain = jnp.clip(1.0 + 0.1 * jax.random.normal(arg_keys[3], (D,), jnp.float32), 0.5, 1.5).astype(jnp.bfloat16)
    w_qkv = draw_w_qkv(jax.random.fold_in(arg_keys[7], 71), 0)
    qk_gain = draw_qk_gain(jax.random.fold_in(arg_keys[7], 71), 0)
    w_out = centred(arg_keys[6], (H, HD, D), (H * HD) ** -0.5, 0.078125, ((0, 8), (2, 4)))
    return dict(patches=patches, w_patch=w_patch, patch_bias=patch_bias, ln_gain=ln_gain, w_qkv=w_qkv, qk_gain=qk_gain, w_out=w_out)


NORM_EPS = 1e-06

def sincos_table(row_ids, col_ids, model_width):
    quarter = model_width // 4
    frequency = 1.0 / 10000.0 ** (jnp.arange(quarter, dtype=jnp.float32) / quarter)
    row_angle = row_ids.astype(jnp.float32)[:, None] * frequency[None, :]
    col_angle = col_ids.astype(jnp.float32)[:, None] * frequency[None, :]
    return jnp.concatenate([jnp.sin(row_angle), jnp.cos(row_angle), jnp.sin(col_angle), jnp.cos(col_angle)], axis=1)

def layer_norm(values, gain_row):
    mean_val = lax.optimization_barrier(jnp.mean(values, axis=-1, keepdims=True))
    centered = values - mean_val
    variance = lax.optimization_barrier(jnp.mean(centered * centered, axis=-1, keepdims=True))
    return centered * lax.rsqrt(variance + NORM_EPS) * gain_row

def reference(patches, w_patch, patch_bias, ln_gain, w_qkv, qk_gain, w_out):
    token_count = GH * GW
    token_ids = jnp.arange(token_count, dtype=jnp.int32)
    flat_pixels = patches.reshape(token_count, PATCH_IN)
    embedded = jnp.dot(flat_pixels, w_patch, preferred_element_type=jnp.float32)
    embedded = embedded + patch_bias.astype(jnp.float32)[None, :] + sincos_table(token_ids // GW, token_ids % GW, D)
    normed = layer_norm(embedded, ln_gain.astype(jnp.float32)).astype(jnp.bfloat16)
    projected = jnp.dot(normed, w_qkv.reshape(D, 3 * H * HD), preferred_element_type=jnp.float32)
    projected = projected.reshape(token_count, 3, H, HD)
    queries = layer_norm(projected[:, 0], qk_gain[0]).astype(jnp.bfloat16)
    keys_all = layer_norm(projected[:, 1], qk_gain[1]).astype(jnp.bfloat16)
    values_all = projected[:, 2].astype(jnp.bfloat16)
    scale_factor = 1.0 / math.sqrt(HD)
    query_block = math.gcd(token_count, 1024)

    def one_head(head_args):
        head_q, head_k, head_v = head_args

        def one_block(block_q):
            scores = jnp.dot(block_q, head_k.T, preferred_element_type=jnp.float32) * scale_factor
            row_peak = lax.optimization_barrier(jnp.max(scores, axis=1, keepdims=True))
            exponent = jnp.exp(scores - row_peak)
            weight_sum = lax.optimization_barrier(jnp.sum(exponent, axis=1, keepdims=True))
            mixed_sum = jnp.dot(exponent.astype(jnp.bfloat16), head_v, preferred_element_type=jnp.float32)
            return (mixed_sum / weight_sum).astype(jnp.bfloat16)
        blocks = lax.map(one_block, head_q.reshape(token_count // query_block, query_block, HD))
        return blocks.reshape(token_count, HD)
    context = lax.map(one_head, (queries.transpose(1, 0, 2), keys_all.transpose(1, 0, 2), values_all.transpose(1, 0, 2)))
    context = context.transpose(1, 0, 2).reshape(token_count, H * HD)
    grouped_ctx = context.reshape(token_count, N_COL, H // N_COL * HD).transpose(1, 0, 2)
    grouped_w = w_out.reshape(N_COL, H // N_COL * HD, D)

    def add_group(running, group_args):
        group_ctx, group_w = group_args
        partial_term = jnp.dot(group_ctx, group_w, preferred_element_type=jnp.float32)
        rounded = lax.optimization_barrier(partial_term.astype(jnp.bfloat16))
        return (running + rounded.astype(jnp.float32), None)
    summed, unused = lax.scan(add_group, jnp.zeros((token_count, D), jnp.float32), (grouped_ctx, grouped_w))
    return summed.astype(jnp.bfloat16)
```

```python
import functools
import math

import jax
import jax.numpy as jnp
from jax import lax
from jax.experimental import pallas as pl
from jax.experimental.pallas import tpu as pltpu
from jax.sharding import PartitionSpec as P

NORM_EPS = 1e-06
KEY_BLOCK = 1024
CHUNKS = 4


def sincos_half(ids, model_width):
    quarter = model_width // 4
    frequency = 1.0 / 10000.0 ** (jnp.arange(quarter, dtype=jnp.float32) / quarter)
    angle = ids.astype(jnp.float32)[:, None] * frequency[None, :]
    return jnp.concatenate([jnp.sin(angle), jnp.cos(angle)], axis=1)


def layer_norm(values, gain_row):
    mean_val = jnp.mean(values, axis=-1, keepdims=True)
    centered = values - mean_val
    variance = jnp.mean(centered * centered, axis=-1, keepdims=True)
    return centered * lax.rsqrt(variance + NORM_EPS) * gain_row


def attention_kernel(key_block, exp_factor, q_ref, k_ref, v_ref, out_ref):
    rows, head_size = math.prod(q_ref.shape[:-1]), q_ref.shape[-1]
    query = q_ref[...].reshape(rows, head_size)
    peak = jnp.full((rows, 1), -1e30, jnp.float32)
    total = jnp.zeros((rows, 1), jnp.float32)
    acc = jnp.zeros((rows, head_size), jnp.float32)
    for start in range(0, k_ref.shape[0], key_block):
        scores = lax.dot_general(
            query,
            k_ref[start : start + key_block, :],
            (((1,), (1,)), ((), ())),
            preferred_element_type=jnp.float32,
        )
        new_peak = jnp.maximum(peak, jnp.max(scores, axis=1, keepdims=True) * exp_factor)
        rescale = jnp.exp2(peak - new_peak)
        weights = jnp.exp2(scores * exp_factor - new_peak)
        total = total * rescale + jnp.sum(weights, axis=1, keepdims=True)
        acc = acc * rescale + jnp.dot(
            weights.astype(jnp.bfloat16),
            v_ref[start : start + key_block, :],
            preferred_element_type=jnp.float32,
        )
        peak = new_peak
    out_ref[...] = (acc / total).astype(out_ref.dtype).reshape(out_ref.shape)


def attention(queries, keys_values, chunk, chunk_rows, width, head_size):
    owners = queries.shape[0]
    heads = width // head_size
    key_count = keys_values.shape[0]
    key_block = math.gcd(key_count, KEY_BLOCK)
    exp_factor = math.log2(math.e) / math.sqrt(head_size)
    rows = owners * chunk_rows
    elements = heads * rows * key_count
    return pl.pallas_call(
        functools.partial(attention_kernel, key_block, exp_factor),
        grid=(heads,),
        in_specs=[
            pl.BlockSpec((owners, chunk_rows, head_size), lambda h: (0, chunk, h)),
            pl.BlockSpec((key_count, head_size), lambda h: (0, h)),
            pl.BlockSpec((key_count, head_size), lambda h: (0, heads + h)),
        ],
        out_specs=pl.BlockSpec((owners, chunk_rows, head_size), lambda h: (0, 0, h)),
        out_shape=jax.ShapeDtypeStruct((owners, chunk_rows, width), jnp.bfloat16),
        compiler_params=pltpu.CompilerParams(
            dimension_semantics=("arbitrary",),
            vmem_limit_bytes=48 * 1024 * 1024,
        ),
        cost_estimate=pl.CostEstimate(
            flops=4 * elements * head_size,
            bytes_accessed=4 * (rows + key_count) * width,
            transcendentals=elements,
        ),
        name="attention",
    )(queries, keys_values, keys_values)


def norm_kernel(x_ref, gain_ref, out_ref):
    out_ref[...] = layer_norm(x_ref[...], gain_ref[...]).astype(out_ref.dtype)


def norm_heads(projected, gain_row, head_size):
    rows, width = projected.shape[0], gain_row.shape[1]
    return pl.pallas_call(
        norm_kernel,
        grid=(width // head_size,),
        in_specs=[
            pl.BlockSpec((rows, head_size), lambda h: (0, h)),
            pl.BlockSpec((1, head_size), lambda h: (0, h)),
        ],
        out_specs=pl.BlockSpec((rows, head_size), lambda h: (0, h)),
        out_shape=jax.ShapeDtypeStruct((rows, width), jnp.bfloat16),
        compiler_params=pltpu.CompilerParams(dimension_semantics=("arbitrary",)),
        cost_estimate=pl.CostEstimate(
            flops=10 * rows * width, bytes_accessed=6 * rows * width, transcendentals=rows
        ),
        name="norm_heads",
    )(projected, gain_row)


def local(patches, w_patch, patch_bias, ln_gain, w_qkv, qk_gain, w_out):
    tile_rows, tile_cols, pixel_width = patches.shape
    model_width = w_patch.shape[1]
    heads_here = w_qkv.shape[2]
    head_size = w_qkv.shape[3]
    col_count = lax.axis_size("col")
    block_tokens = tile_rows * tile_cols * col_count
    row_anchor = lax.axis_index("row") * tile_rows
    qkv_matrix = w_qkv.reshape(model_width, 3 * heads_here * head_size)
    bias_row = patch_bias.astype(jnp.float32)[None, :]
    gain_row = ln_gain.astype(jnp.float32)
    pixels = lax.all_gather(patches, "col", axis=1, tiled=True)
    piece_cols = pixels.shape[1]
    flat_pixels = pixels.reshape(tile_rows * piece_cols, pixel_width)
    embedded = jnp.dot(flat_pixels, w_patch, preferred_element_type=jnp.float32) + bias_row
    row_half = sincos_half(row_anchor + jnp.arange(tile_rows, dtype=jnp.int32), model_width)
    col_half = sincos_half(jnp.arange(piece_cols, dtype=jnp.int32), model_width)
    row_half, col_half = lax.optimization_barrier((row_half, col_half))
    half_shape = (tile_rows, piece_cols, model_width // 2)
    position = jnp.concatenate(
        [
            jnp.broadcast_to(row_half[:, None, :], half_shape),
            jnp.broadcast_to(col_half[None, :, :], half_shape),
        ],
        axis=2,
    )
    embedded = embedded + position.reshape(tile_rows * piece_cols, model_width)
    normed = layer_norm(embedded, gain_row).astype(jnp.bfloat16)
    normed_piece = normed.reshape(tile_rows, piece_cols, model_width)
    project_piece_cols = normed_piece.shape[1]
    flat_normed = normed_piece.reshape(tile_rows * project_piece_cols, model_width)
    projected = jnp.dot(flat_normed, qkv_matrix, preferred_element_type=jnp.float32)
    head_width = heads_here * head_size
    gain_qk = qk_gain.reshape(1, 2 * head_width)
    normed_qk = norm_heads(projected, gain_qk, head_size)
    keys_values = jnp.concatenate(
        [normed_qk[:, head_width:], projected[:, 2 * head_width :].astype(jnp.bfloat16)], axis=1
    )
    keys_values = lax.all_gather(keys_values, "row", axis=0, tiled=True)
    out_weight = lax.all_gather(w_out, "row", axis=2, tiled=True).reshape(
        heads_here * head_size, model_width
    )
    owned = block_tokens // col_count
    chunk_rows = owned // math.gcd(owned // 16, CHUNKS)
    queries = normed_qk.reshape(col_count, owned, 2 * head_width)
    pieces = []
    for chunk in range(owned // chunk_rows):
        context = attention(queries, keys_values, chunk, chunk_rows, head_width, head_size)
        partial = jnp.dot(
            context.reshape(col_count * chunk_rows, head_width),
            out_weight,
            preferred_element_type=jnp.float32,
        ).astype(jnp.bfloat16)
        pieces.append(lax.psum_scatter(partial, "col", scatter_dimension=0, tiled=True))
    return jnp.concatenate(pieces, axis=0)


def solution(mesh):
    return jax.shard_map(
        local,
        mesh=mesh,
        in_specs=(
            P("row", "col", None),
            P(),
            P(),
            P(),
            P(None, None, "col", None),
            P(None, "col", None),
            P("col", None, "row"),
        ),
        out_specs=P(("row", "col"), None),
        check_vma=False,
    )
```
